128 devices in a mesh: dp: 32 (over x, z, core), tp: 4 (over y).
Axes of the slice: x: 4, y: 4, z: 4, core: 2. Of those that a mesh axis runs over, the one named last changes fastest.
Arguments:
- hidden_in: bfloat16 [2048, 3584], P(('dp', 'tp')), may hold values from -6 to 6
- query_latent: bfloat16 [2048, 64, 512], P(('dp', 'tp')), may hold values from -348 to 347
- query_rope: bfloat16 [2048, 4096], P(('dp', 'tp')), may hold values from -348 to 347
- cache_latent: bfloat16 [2048, 128, 512], P(('dp', 'tp')), may hold values from -6 to 6
- cache_rope: bfloat16 [2048, 64, 128], P(('dp', 'tp')), may hold values from -6 to 6
- lengths: int32 [2048], P(('dp', 'tp')), may hold values from 16 to 128
- value_up: bfloat16 [512, 4096], P(None, 'tp'), may hold values from -1 to 1
- out_proj: bfloat16 [4096, 3584], P('tp'), may hold values from -0.09375 to 0.09375
- norm_gain: float32 [3584], replicated, may hold values from 0.1 to 1.9
- expert_gate: bfloat16 [128, 3584, 1024], P(('dp', 'tp')), may hold values from -0.09375 to 0.09375
- expert_down: bfloat16 [128, 1024, 3584], P(('dp', 'tp')), may hold values from -0.1875 to 0.1875
- expert_ids: int32 [2048, 8], P(('dp', 'tp')), may hold values from 0 to 127, all different within a row; in each aligned block of 16 rows (0 to 15, 16 to 31, ...) at most 2 rows name the same one
- affinity: float32 [2048, 8], P(('dp', 'tp')), may hold values from 0.05 to 1
Outputs:
- layer_out: bfloat16 [2048, 3584], P(('dp', 'tp'))
The draws below stay inside these ranges and needn't reach their ends.
Inputs may be any that keep to these rules, and one draw needn't show every extreme that they name: `expert_ids`: in each aligned block of 16 rows (the rows of one device) no expert is named by more than 2 rows.
All inputs are finite; a program needn't handle non-finite values.
Results may differ from the reference program's by a relative error of at most 0.0081.
Values may be sent and summed in bfloat16 or wider, within the bound.
No kernel may reach another device: no remote copies, remote signals or barrier semaphores. Data moves between devices by JAX's collectives and lax.ppermute only.
A program may use at most 128 MiB of HBM per device.

```python
import math
import jax
import jax.numpy as jnp
import numpy as np
from jax import lax

D = 3584
HEADS = 64
LAT = 512
ROPE = 64
HEAD_V = 64
FF = 1024
TOPK = 8
CTX = 128
TOK_DEV = 16
TOKENS = 2048
EXPERTS = 128
CAP = 2


def key_parts(key):
    latent = jax.random.normal(jax.random.fold_in(key, 101), (TOKENS, CTX, LAT), jnp.float32)
    rotary = jax.random.normal(jax.random.fold_in(key, 102), (TOKENS, ROPE, CTX), jnp.float32)
    latent = jnp.clip(latent, -6.0, 6.0).astype(jnp.bfloat16).astype(jnp.float32)
    rotary = jnp.clip(rotary, -6.0, 6.0).astype(jnp.bfloat16).astype(jnp.float32)
    return (latent, rotary)


def draw_cache_latent(key, part):
    return key_parts(key)[0].astype(jnp.bfloat16)


def draw_cache_rope(key, part):
    return key_parts(key)[1].astype(jnp.bfloat16)


def query_parts(key):
    full_shape = (TOKENS, HEADS, LAT + ROPE)
    return jnp.clip(jax.random.normal(jax.random.fold_in(key, 103), full_shape, jnp.float32), -6.0, 6.0)


def draw_query_latent(key, part):
    return query_parts(key)[:, :, :LAT].astype(jnp.bfloat16)


def draw_query_rope(key, part):
    return query_parts(key)[:, :, LAT:].reshape(TOKENS, HEADS * ROPE).astype(jnp.bfloat16)


def plant(result, rng, smallest, high):
    spot = [jax.random.randint(jax.random.fold_in(rng, axis), (), 0, length) for axis, length in enumerate(result.shape)]
    main_axis = result.shape.index(max(result.shape))
    beside = spot[:main_axis] + [(spot[main_axis] + 1) % result.shape[main_axis]] + spot[main_axis + 1:]
    return result.at[tuple(spot)].set(smallest).at[tuple(beside)].set(high)


def shard_levels(own_key, extent, pieces, smallest, top_value):
    def one(axis_at, shards_of):
        draws = jax.random.uniform(jax.random.fold_in(jax.random.fold_in(own_key, 6), axis_at), (shards_of,), jnp.float32, smallest / len(pieces), top_value / len(pieces))
        return jnp.repeat(jnp.exp(draws), extent[axis_at] // shards_of).reshape((-1,) + (1,) * (len(extent) - axis_at - 1))

    level = one(*pieces[0])
    for cut in pieces[1:]:
        level = level * one(*cut)
    return level


def shared_out(key, own, number, rows, number_of, top, limit, slope):
    sequence = jax.random.permutation(key, number_of)
    heavy_load, common = load_shares(number_of, rows * top, limit, slope, True), load_shares(number_of, rows * top, limit, slope, False)
    places = jnp.arange(number_of)

    def named(tallies, rotation):
        used = int((tallies > 0).sum())
        fixed = max(1, used // 4)
        moved = fixed + (places - fixed + rotation * (used - fixed)) % max(1, number_of - fixed)
        return jnp.zeros((number_of,), jnp.int32).at[sequence[jnp.where(places < fixed, places, moved)]].set(jnp.asarray(tallies, jnp.int32))

    tallies = jnp.where(number % 4 == 0, named(heavy_load, number // 4), named(common, number - number // 4 - 1))
    mixed = jax.random.permutation(jax.random.fold_in(own, 3), number_of)
    source_of, receiver = mixed[0:number_of // 2 * 2:2], mixed[1:number_of // 2 * 2:2]
    room = jnp.minimum(tallies[source_of] - 1, limit - tallies[receiver]) // 2
    room = jnp.where((source_of == sequence[0]) | (receiver == sequence[0]) | (tallies[receiver] == 0), 0, jnp.maximum(room, 0))
    moved = jax.random.randint(jax.random.fold_in(own, 4), (number_of // 2,), 0, 1 << 20) % (room + 1)
    tallies = tallies.at[source_of].add(-moved).at[receiver].add(moved)
    labels = jnp.searchsorted(jnp.cumsum(tallies), jnp.arange(rows * top), side="right").astype(jnp.int32)
    grid = labels.reshape(top, rows).T
    grid = grid[jax.random.permutation(jax.random.fold_in(own, 1), rows)]
    rotation = jax.random.randint(jax.random.fold_in(own, 2), (rows, 1), 0, top)
    return jnp.take_along_axis(grid, (jnp.arange(top)[None, :] + rotation) % top, axis=1)


def load_shares(count, total, reach, slope, full):
    weights = [(1 << 20) // math.isqrt(standing ** slope) + 1 for standing in range(1, count + 1)]
    largest = reach if full else min(reach, max(-(-total // count), total * weights[0] // sum(weights)))
    least = 1 if total - largest >= count - 1 else 0
    given, surplus = [largest] + [least] * (count - 1), total - largest - least * (count - 1)
    while surplus > 0:
        free = [i for i in range(1, count) if given[i] < largest] or [i for i in range(1, count) if given[i] < reach]
        mass, remaining = sum([weights[i] for i in free]), surplus
        for i in free:
            addition = min(reach - given[i], max(1, remaining * weights[i] // mass), surplus)
            given[i] = given[i] + addition
            surplus = surplus - addition
    return np.array(given)


def gaussian(own_key, shape, width, limit, shards=(), kind=jnp.bfloat16):
    factor_of = shard_levels(own_key, shape, shards, -0.22, 0.18) if shards else 1.0
    values = jax.random.normal(own_key, shape, jnp.float32) * width * factor_of
    return jnp.minimum(jnp.maximum(values, -limit), limit).astype(kind)


def setup_inputs(seed: int = 0) -> dict:
    key_list = jax.random.split(jax.random.key(seed), 14)
    hidden_in = gaussian(key_list[0], (TOKENS, D), 1.0, 6.0, ((0, 128),))
    query_latent = draw_query_latent(jax.random.fold_in(key_list[13], 71), 0)
    query_rope = draw_query_rope(jax.random.fold_in(key_list[13], 71), 0)
    cache_latent = draw_cache_latent(jax.random.fold_in(key_list[13], 71), 0)
    cache_rope = draw_cache_rope(jax.random.fold_in(key_list[13], 71), 0)
    lengths = plant(jax.random.randint(key_list[5], (TOKENS,), CTX // 8, CTX + 1), jax.random.fold_in(key_list[5], 1), CTX // 8, CTX).astype(jnp.int32)
    value_up = gaussian(key_list[6], (LAT, HEADS * HEAD_V), (LAT // 16) ** -0.5, 1.0, ((1, 4),))
    out_proj = gaussian(key_list[7], (HEADS * HEAD_V, D), (HEADS * HEAD_V) ** -0.5, 0.09375, ((0, 4),))
    norm_gain = jnp.clip(1.0 + 0.18 * jax.random.normal(key_list[8], (D,), jnp.float32), 0.1, 1.9)
    expert_gate = gaussian(key_list[9], (EXPERTS, D, FF), D ** -0.5, 0.09375, ((0, 128),))
    expert_down = gaussian(key_list[10], (EXPERTS, FF, D), FF ** -0.5, 0.1875, ((0, 128),))
    expert_ids_keys = jax.random.split(jax.random.fold_in(key_list[11], 1), TOKENS // TOK_DEV)
    expert_ids_turns = jax.random.permutation(jax.random.fold_in(key_list[11], 3), TOKENS // TOK_DEV)
    expert_ids = jax.vmap(lambda own, number: shared_out(jax.random.fold_in(key_list[11], 2), own, number, TOK_DEV, EXPERTS, TOPK, CAP, 2))(expert_ids_keys, expert_ids_turns).reshape((TOKENS, TOPK))
    affinity = jnp.clip(jnp.exp(math.log(1.0) - 2.9957323 * jax.random.uniform(key_list[12], (TOKENS, TOPK), jnp.float32) ** shard_levels(key_list[12], (TOKENS, TOPK), ((0, 128),), -0.2, 0.2)), 0.05, 1.0)
    return dict(hidden_in=hidden_in, query_latent=query_latent, query_rope=query_rope, cache_latent=cache_latent, cache_rope=cache_rope, lengths=lengths, value_up=value_up, out_proj=out_proj, norm_gain=norm_gain, expert_gate=expert_gate, expert_down=expert_down, expert_ids=expert_ids, affinity=affinity)


score_scale = 192.0 ** (-0.5)
norm_eps = 1e-06
route_scale = 2.5

def attend(query_latent, query_rope, cache_latent, cache_rope, lengths):
    token_count, head_count, latent_width = query_latent.shape
    rope_width = cache_rope.shape[1]
    context = cache_latent.shape[1]
    latent_wide = cache_latent.astype(jnp.float32)
    query_rot = query_rope.astype(jnp.float32).reshape(token_count, head_count, rope_width)
    scores = jnp.einsum('thl,tpl->thp', query_latent.astype(jnp.float32), latent_wide)
    scores = scores + jnp.einsum('thr,trp->thp', query_rot, cache_rope.astype(jnp.float32))
    scores = scores * score_scale
    position = lax.broadcasted_iota(jnp.int32, (token_count, 1, context), 2)
    scores = jnp.where(position < lengths.astype(jnp.int32)[:, None, None], scores, -jnp.inf)
    row_max = lax.optimization_barrier(jnp.max(scores, axis=2, keepdims=True))
    raised = jnp.exp(scores - row_max)
    attn_weights = (raised / lax.optimization_barrier(jnp.sum(raised, axis=2, keepdims=True))).astype(jnp.bfloat16)
    latent_out = jnp.einsum('thp,tpl->thl', attn_weights.astype(jnp.float32), latent_wide)
    return latent_out.astype(jnp.bfloat16)

def reference(hidden_in, query_latent, query_rope, cache_latent, cache_rope, lengths, value_up, out_proj, norm_gain, expert_gate, expert_down, expert_ids, affinity):
    latent_out = attend(query_latent, query_rope, cache_latent, cache_rope, lengths)
    up_table = value_up.astype(jnp.float32).reshape(LAT, HEADS, HEAD_V)
    per_head = jnp.einsum('thl,lhv->thv', latent_out.astype(jnp.float32), up_table).astype(jnp.bfloat16)
    attn_sum = jnp.dot(per_head.reshape(TOKENS, HEADS * HEAD_V), out_proj, preferred_element_type=jnp.float32)
    hidden = (hidden_in.astype(jnp.float32) + attn_sum).astype(jnp.bfloat16)
    wide_hidden = hidden.astype(jnp.float32)
    inv_norm = lax.rsqrt(lax.optimization_barrier(jnp.mean(wide_hidden * wide_hidden, axis=1, keepdims=True)) + norm_eps)
    normed = (wide_hidden * inv_norm * norm_gain.astype(jnp.float32)).astype(jnp.bfloat16)
    blocks = TOKENS // TOK_DEV
    per_block = TOK_DEV * TOPK
    block_ids = expert_ids.astype(jnp.int32).reshape(blocks, per_block)
    expert_iota = jnp.arange(EXPERTS, dtype=jnp.int32)
    one_hot = (block_ids[:, :, None] == expert_iota[None, None, :]).astype(jnp.int32)
    earlier = jnp.cumsum(one_hot, axis=1) - one_hot
    slot_index = lax.optimization_barrier(jnp.sum(earlier * one_hot, axis=2)).astype(jnp.int32)
    block_number = jnp.arange(blocks, dtype=jnp.int32)[:, None]
    target = (block_ids * (blocks * CAP) + block_number * CAP + slot_index).reshape(-1)
    owner_row = jnp.arange(TOKENS * TOPK, dtype=jnp.int32) // TOPK
    route_weight = route_scale * affinity / lax.optimization_barrier(jnp.sum(affinity, axis=1, keepdims=True))
    source_row = jnp.full((EXPERTS * blocks * CAP,), TOKENS, jnp.int32).at[target].set(owner_row)
    row_weight = jnp.zeros((EXPERTS * blocks * CAP,), jnp.float32).at[target].set(route_weight.reshape(-1))
    padded = jnp.concatenate([normed, jnp.zeros((1, D), jnp.bfloat16)], axis=0)

    def one_expert(total, inputs):
        rows_here, weights_here, gate_here, down_here = inputs
        inner_act = jax.nn.silu(jnp.dot(padded[rows_here], gate_here, preferred_element_type=jnp.float32)).astype(jnp.bfloat16)
        answer = jnp.dot(inner_act, down_here, preferred_element_type=jnp.float32).astype(jnp.bfloat16).astype(jnp.float32)
        return (total.at[rows_here].add(weights_here[:, None] * answer, mode='drop'), None)
    moe_sum = lax.scan(one_expert, jnp.zeros((TOKENS, D), jnp.float32), (source_row.reshape(EXPERTS, -1), row_weight.reshape(EXPERTS, -1), expert_gate, expert_down))[0]
    return (wide_hidden + moe_sum).astype(jnp.bfloat16)
```

```python
import jax
import jax.numpy as jnp
from jax import lax
from jax.experimental import pallas as pl
from jax.experimental.pallas import tpu as pltpu
from jax.sharding import PartitionSpec as P

score_scale = 192.0 ** (-0.5)
norm_eps = 1e-06
route_scale = 2.5
bf16 = jnp.bfloat16
f32 = jnp.float32


TP = 4
SLOTS = 2
QUARTERS = 4
SHIFTS = (0, 1, 2, 3)


def nn(a, b):
    return lax.dot_general(a, b, (((1,), (0,)), ((), ())), preferred_element_type=f32)


def nt(a, b):
    return lax.dot_general(a, b, (((1,), (1,)), ((), ())), preferred_element_type=f32)


def attend(lengths, mine, query_latent, query_rope, cache_latent, cache_rope, block):
    tokens, heads, latent = query_latent.shape
    context = cache_latent.shape[1]
    rope = cache_rope.shape[1]
    group = heads // TP
    steps = tokens // block
    pairs = heads * rope // 128

    def body(len_ref, mine_ref, q_ref, qr_ref, c_ref, cr_ref, o0, o1, o2, o3, qr_scr, out_scr):
        step = pl.program_id(0)

        @pl.when(step == 0)
        def _():
            for j in range(pairs):
                pair = qr_ref[:, 128 * j : 128 * (j + 1)].astype(f32)
                qr_scr[pl.ds(2 * j, tokens, stride=heads), :] = pair
                qr_scr[pl.ds(2 * j + 1, tokens, stride=heads), :] = pltpu.roll(pair, 128 - rope, 1)

        position = lax.broadcasted_iota(jnp.int32, (heads, context), 1)
        for i in range(block):
            token = step * block + i
            keys = c_ref[i]
            rot = qr_scr[pl.ds(pl.multiple_of(token * heads, heads), heads), :][:, :rope].astype(bf16)
            scores = nt(q_ref[i], keys) + nn(rot, cr_ref[i])
            scores = jnp.where(position < len_ref[token], scores * score_scale, -jnp.inf)
            raised = jnp.exp(scores - jnp.max(scores, axis=1, keepdims=True))
            weights = (raised / jnp.sum(raised, axis=1, keepdims=True)).astype(bf16)
            mixed = nn(weights, keys)
            for c in range(latent // 128):
                out_scr[c, pl.ds(token, heads, stride=tokens), :] = mixed[:, 128 * c : 128 * (c + 1)]

        @pl.when(step == steps - 1)
        def _():
            for shift, o in zip(SHIFTS, (o0, o1, o2, o3)):
                first = ((mine_ref[0] + shift) % TP) * (group * tokens)
                for c in range(latent // 128):
                    rows = out_scr[c, pl.ds(pl.multiple_of(first, group * tokens), group * tokens), :]
                    o[:, 128 * c : 128 * (c + 1)] = rows.astype(bf16)

    out = jax.ShapeDtypeStruct((group * tokens, latent), bf16)
    return pl.pallas_call(
        body,
        out_shape=[out] * TP,
        grid_spec=pltpu.PrefetchScalarGridSpec(
            num_scalar_prefetch=2,
            grid=(steps,),
            in_specs=[
                pl.BlockSpec((block, heads, latent), lambda i, *_: (i, 0, 0)),
                pl.BlockSpec((tokens, heads * rope), lambda i, *_: (0, 0)),
                pl.BlockSpec((block, context, latent), lambda i, *_: (i, 0, 0)),
                pl.BlockSpec((block, rope, context), lambda i, *_: (i, 0, 0)),
            ],
            out_specs=[pl.BlockSpec((group * tokens, latent), lambda i, *_: (0, 0))] * TP,
            scratch_shapes=[
                pltpu.VMEM((tokens * heads, 128), f32),
                pltpu.VMEM((latent // 128, heads * tokens, 128), f32),
            ],
        ),
        compiler_params=pltpu.CompilerParams(vmem_limit_bytes=24 << 20),
        name="attend",
    )(lengths, mine, query_latent, query_rope, cache_latent, cache_rope)


def project(parts, value_up, out_proj, tokens, block):
    latent, up_width = value_up.shape
    width = out_proj.shape[1]
    head_v = up_width * tokens // parts[0].shape[0]
    pair_count = up_width // 128

    def body(l0, l1, l2, l3, up_ref, w_ref, o0, o1, o2, o3, ph_scr):
        parts_ref = (l0, l1, l2, l3)

        @pl.when(pl.program_id(0) == 0)
        def _():
            low = lax.broadcasted_iota(jnp.int32, (TP * tokens, 128), 1) < head_v
            for j in range(pair_count):
                rows = [r[(2 * j + half) * tokens : (2 * j + half + 1) * tokens, :] for half in (0, 1) for r in parts_ref]
                both = nn(jnp.concatenate(rows, axis=0), up_ref[:, 128 * j : 128 * (j + 1)])
                half_rows = TP * tokens
                ph_scr[:, 128 * j : 128 * (j + 1)] = jnp.where(low, both[:half_rows], both[half_rows:]).astype(bf16)

        total = nn(ph_scr[...], w_ref[...])
        o0[...] = total[:tokens]
        for i, o in enumerate((o1, o2, o3)):
            o[...] = total[(i + 1) * tokens : (i + 2) * tokens].astype(bf16)

    rows = parts[0].shape[0]
    return pl.pallas_call(
        body,
        grid=(width // block,),
        out_shape=[jax.ShapeDtypeStruct((tokens, width), f32)] + [jax.ShapeDtypeStruct((tokens, width), bf16)] * 3,
        in_specs=[pl.BlockSpec((rows, latent), lambda i: (0, 0))] * TP
        + [pl.BlockSpec((latent, up_width), lambda i: (0, 0)), pl.BlockSpec((up_width, block), lambda i: (0, i))],
        out_specs=[pl.BlockSpec((tokens, block), lambda i: (0, i))] * TP,
        scratch_shapes=[pltpu.VMEM((TP * tokens, up_width), bf16)],
        compiler_params=pltpu.CompilerParams(vmem_limit_bytes=16 << 20),
        name="project",
    )(*parts, value_up, out_proj)


def route(expert_ids, affinity, experts):
    tokens, top = expert_ids.shape
    per_expert = SLOTS * QUARTERS
    columns = experts * per_expert

    def body(id_ref, aff_ref, pick_ref, weight_ref):
        expert = lax.broadcasted_iota(jnp.int32, (tokens, experts), 1)
        aff = aff_ref[...]
        weight = route_scale * aff / jnp.sum(aff, axis=1, keepdims=True)
        named = jnp.zeros((tokens, experts), f32)
        spread = jnp.zeros((tokens, experts), f32)
        for k in range(top):
            here = id_ref[:, k : k + 1] == expert
            named = named + jnp.where(here, 1.0, 0.0)
            spread = spread + jnp.where(here, weight[:, k : k + 1], 0.0)
        above = lax.broadcasted_iota(jnp.int32, (tokens, tokens), 0) > lax.broadcasted_iota(jnp.int32, (tokens, tokens), 1)
        earlier = nn(above.astype(f32).astype(bf16), named.astype(bf16))
        column = lax.broadcasted_iota(jnp.int32, (experts, columns), 1)
        widen = (column // per_expert == lax.broadcasted_iota(jnp.int32, (experts, columns), 0)).astype(f32).astype(bf16)
        named_wide = nn(named.astype(bf16), widen)
        earlier_wide = nn(earlier.astype(bf16), widen)
        high = spread.astype(bf16)
        low = (spread - high.astype(f32)).astype(bf16)
        high_wide = nn(high, widen)
        low_wide = nn(low, widen)
        at = lax.broadcasted_iota(jnp.int32, (tokens, columns), 1)
        slot = ((at // QUARTERS) % SLOTS).astype(f32)
        taken = jnp.logical_and(named_wide > 0.5, earlier_wide == slot)
        picks = []
        for q in range(QUARTERS):
            here = jnp.logical_and(taken, at % QUARTERS == q)
            picks.append(jnp.where(here, 1.0, 0.0))
            weight_ref[q * tokens : (q + 1) * tokens, :] = jnp.where(here, high_wide, 0.0).astype(bf16)
            weight_ref[(QUARTERS + q) * tokens : (QUARTERS + q + 1) * tokens, :] = jnp.where(here, low_wide, 0.0).astype(bf16)
        pick_ref[...] = jnp.concatenate(picks, axis=0).T.astype(bf16)

    return pl.pallas_call(
        body,
        out_shape=[
            jax.ShapeDtypeStruct((columns, QUARTERS * tokens), bf16),
            jax.ShapeDtypeStruct((2 * QUARTERS * tokens, columns), bf16),
        ],
        compiler_params=pltpu.CompilerParams(vmem_limit_bytes=8 << 20),
        name="route",
    )(expert_ids, affinity)


def norm_dispatch(own, parts, hidden_in, norm_gain, pick):
    tokens, width = hidden_in.shape
    quarter = width // QUARTERS

    def body(own_ref, p1, p2, p3, h_ref, g_ref, pick_ref, hid_ref, out_ref):
        total = own_ref[...] + p1[...].astype(f32) + p2[...].astype(f32) + p3[...].astype(f32)
        hidden = (h_ref[...].astype(f32) + total).astype(bf16)
        hid_ref[...] = hidden
        wide = hidden.astype(f32)
        inv = lax.rsqrt(jnp.sum(wide * wide, axis=1, keepdims=True) * (1.0 / width) + norm_eps)
        normed = (wide * inv * g_ref[...]).astype(bf16)
        stacked = jnp.concatenate([normed[:, q * quarter : (q + 1) * quarter] for q in range(QUARTERS)], axis=0)
        out_ref[...] = nn(pick_ref[...], stacked).astype(bf16)

    return pl.pallas_call(
        body,
        out_shape=[
            jax.ShapeDtypeStruct((tokens, width), bf16),
            jax.ShapeDtypeStruct((pick.shape[0], quarter), bf16),
        ],
        compiler_params=pltpu.CompilerParams(vmem_limit_bytes=16 << 20),
        name="norm_dispatch",
    )(own, *parts, hidden_in, norm_gain, pick)


def run_expert(rows, gate, down):
    total, quarter = rows.shape
    count = total // QUARTERS
    hidden_units = gate.shape[1]

    def body(r_ref, g_ref, d_ref, o_ref, wide_scr, acc_scr, act_scr):
        step = pl.program_id(0)
        lanes = quarter // 128

        @pl.when(step == 0)
        def _():
            for c in range(lanes):
                wide_scr[c] = r_ref[:, 128 * c : 128 * (c + 1)].astype(f32)

        @pl.when(step < QUARTERS)
        def _():
            lhs = jnp.concatenate(
                [wide_scr[c, pl.ds(step, count, stride=QUARTERS), :].astype(bf16) for c in range(lanes)], axis=1
            )
            part = nn(lhs, g_ref[...])

            @pl.when(step == 0)
            def _():
                acc_scr[...] = part

            @pl.when(step > 0)
            def _():
                acc_scr[...] += part

            @pl.when(step == QUARTERS - 1)
            def _():
                inner = acc_scr[...]
                act_scr[...] = (inner / (1.0 + jnp.exp(-inner))).astype(bf16)

        @pl.when(step >= QUARTERS)
        def _():
            part = nn(act_scr[...], d_ref[...])
            for c in range(lanes):
                wide_scr[c, pl.ds(step - QUARTERS, count, stride=QUARTERS), :] = part[:, 128 * c : 128 * (c + 1)]

            @pl.when(step == 2 * QUARTERS - 1)
            def _():
                for c in range(lanes):
                    o_ref[:, 128 * c : 128 * (c + 1)] = wide_scr[c].astype(bf16)

    return pl.pallas_call(
        body,
        grid=(2 * QUARTERS,),
        out_shape=jax.ShapeDtypeStruct((total, quarter), bf16),
        in_specs=[
            pl.BlockSpec((total, quarter), lambda i: (0, 0)),
            pl.BlockSpec((quarter, hidden_units), lambda i: (jnp.minimum(i, QUARTERS - 1), 0)),
            pl.BlockSpec((hidden_units, quarter), lambda i: (0, jnp.maximum(i - QUARTERS, 0))),
        ],
        out_specs=pl.BlockSpec((total, quarter), lambda i: (0, 0)),
        scratch_shapes=[
            pltpu.VMEM((quarter // 128, total, 128), f32),
            pltpu.VMEM((count, hidden_units), f32),
            pltpu.VMEM((count, hidden_units), bf16),
        ],
        compiler_params=pltpu.CompilerParams(vmem_limit_bytes=32 << 20),
        name="run_expert",
    )(rows, gate, down)


def combine(rows, weight, hidden):
    tokens, width = hidden.shape
    quarter = width // QUARTERS

    def body(r_ref, w_ref, h_ref, o_ref):
        both = nn(w_ref[...], r_ref[...])
        half = QUARTERS * tokens
        moe = both[:half] + both[half:]
        for q in range(QUARTERS):
            at = slice(q * quarter, (q + 1) * quarter)
            o_ref[:, at] = (h_ref[:, at].astype(f32) + moe[q * tokens : (q + 1) * tokens]).astype(bf16)

    return pl.pallas_call(
        body,
        out_shape=jax.ShapeDtypeStruct((tokens, width), bf16),
        compiler_params=pltpu.CompilerParams(vmem_limit_bytes=16 << 20),
        name="combine",
    )(rows, weight, hidden)


def per_device(
    hidden_in,
    query_latent,
    query_rope,
    cache_latent,
    cache_rope,
    lengths,
    value_up,
    out_proj,
    norm_gain,
    expert_gate,
    expert_down,
    expert_ids,
    affinity,
):
    tokens, width = hidden_in.shape
    experts = lax.axis_size("dp") * lax.axis_size("tp")
    mine = lax.axis_index("tp").astype(jnp.int32).reshape(1)

    def shifted(array, shift):
        return lax.ppermute(array, "tp", [(i, (i + shift) % TP) for i in range(TP)])

    pick, weight = route(expert_ids, affinity, experts)
    by_shift = attend(lengths, mine, query_latent, query_rope, cache_latent, cache_rope, 4)
    latents = [by_shift[0]] + [shifted(by_shift[s], s) for s in SHIFTS[1:]]
    sums = project(latents, value_up, out_proj, tokens, 512)
    parts = [shifted(sums[s], -s) for s in SHIFTS[1:]]
    hidden, outgoing = norm_dispatch(sums[0], parts, hidden_in, norm_gain.reshape(1, width), pick)

    def exchange(rows):
        cut = rows.reshape(experts, SLOTS * QUARTERS, width // QUARTERS)
        return lax.all_to_all(cut, ("dp", "tp"), 0, 0, tiled=True).reshape(rows.shape)

    answer = run_expert(exchange(outgoing), expert_gate[0], expert_down[0])
    return combine(exchange(answer), weight, hidden)


def solution(mesh):
    return jax.shard_map(
        per_device,
        mesh=mesh,
        in_specs=(
            P(("dp", "tp"), None),
            P(("dp", "tp"), None, None),
            P(("dp", "tp"), None),
            P(("dp", "tp"), None, None),
            P(("dp", "tp"), None, None),
            P(("dp", "tp")),
            P(None, "tp"),
            P("tp", None),
            P(),
            P(("dp", "tp"), None, None),
            P(("dp", "tp"), None, None),
            P(("dp", "tp"), None),
            P(("dp", "tp"), None),
        ),
        out_specs=P(("dp", "tp"), None),
        check_vma=False,
    )
```

```python
import jax
import jax.numpy as jnp
from jax import lax
from jax.experimental import pallas as pl
from jax.experimental.pallas import tpu as pltpu
from jax.sharding import PartitionSpec as P

score_scale = 192.0 ** (-0.5)
norm_eps = 1e-06
route_scale = 2.5
bf16 = jnp.bfloat16
f32 = jnp.float32


TP = 4
SLOTS = 2
QUARTERS = 4
SHIFTS = (0, 2, 1, 3)


def nn(a, b):
    return lax.dot_general(a, b, (((1,), (0,)), ((), ())), preferred_element_type=f32)


def nt(a, b):
    return lax.dot_general(a, b, (((1,), (1,)), ((), ())), preferred_element_type=f32)


def in_hbm(array):
    return pltpu.with_memory_space_constraint(array, pltpu.HBM)


def attend(lengths, mine, query_latent, query_rope, cache_latent, cache_rope, table, block):
    tokens, heads, latent = query_latent.shape
    context = cache_latent.shape[1]
    rope = cache_rope.shape[1]
    group = heads // TP
    steps = tokens // block
    pairs = heads * rope // 128

    def body(len_ref, mine_ref, q_ref, qr_ref, c_ref, cr_ref, t_ref, o0, o1, o2, o3, copied, qr_scr, w_scr, sem):
        step = pl.program_id(0)
        fetch = pltpu.make_async_copy(t_ref, copied, sem)

        @pl.when(step == 0)
        def _():
            fetch.start()

        for j in range(pairs):
            pair = qr_ref[:, 128 * j : 128 * (j + 1)].astype(f32)
            qr_scr[pl.ds(2 * j, block, stride=heads), :] = pair
            qr_scr[pl.ds(2 * j + 1, block, stride=heads), :] = pltpu.roll(pair, 128 - rope, 1)
        position = lax.broadcasted_iota(jnp.int32, (heads, context), 1)
        for i in range(0, block, 2):
            both = nt(q_ref[i : i + 2].reshape(2 * heads, latent), c_ref[i : i + 2].reshape(2 * context, latent))
            for k in (0, 1):
                t = i + k
                rot = qr_scr[t * heads : (t + 1) * heads, :rope].astype(bf16)
                scores = both[k * heads : (k + 1) * heads, k * context : (k + 1) * context] + nn(rot, cr_ref[t])
                live = position < len_ref[step * block + t]
                w_scr[pl.ds(t, heads, stride=block), :] = jnp.where(live, scores * score_scale, -jnp.inf)
        scores = w_scr[...]
        raised = jnp.exp(scores - jnp.max(scores, axis=1, keepdims=True))
        weights = (raised / jnp.sum(raised, axis=1, keepdims=True)).astype(bf16)
        token = lax.broadcasted_iota(jnp.int32, (heads * block, context), 0) % block
        spread = jnp.concatenate([jnp.where(token == i, weights, jnp.zeros_like(weights)) for i in range(block)], axis=1)
        mixed = nn(spread, c_ref[...].reshape(block * context, latent)).reshape(heads, block, latent).astype(bf16)
        first_token = pl.multiple_of(step * block, block)
        for g in range(TP):
            for shift, o in zip(SHIFTS, (o0, o1, o2, o3)):

                @pl.when((mine_ref[0] + shift) % TP == g)
                def _():
                    o[:, pl.ds(first_token, block), :] = mixed[g * group : (g + 1) * group]

        @pl.when(step == steps - 1)
        def _():
            fetch.wait()

    out = jax.ShapeDtypeStruct((group, tokens, latent), bf16)
    *parts, copied = pl.pallas_call(
        body,
        out_shape=[out] * TP + [pltpu.VMEM(table.shape, bf16)],
        grid=(steps,),
        in_specs=[
            pl.BlockSpec((tokens,), lambda i: (0,), memory_space=pltpu.SMEM),
            pl.BlockSpec(memory_space=pltpu.SMEM),
            pl.BlockSpec((block, heads, latent), lambda i: (i, 0, 0)),
            pl.BlockSpec((block, heads * rope), lambda i: (i, 0)),
            pl.BlockSpec((block, context, latent), lambda i: (i, 0, 0)),
            pl.BlockSpec((block, rope, context), lambda i: (i, 0, 0)),
            pl.BlockSpec(memory_space=pl.ANY),
        ],
        out_specs=[pl.BlockSpec((group, tokens, latent), lambda i: (0, 0, 0))] * TP + [pl.BlockSpec(memory_space=pl.ANY)],
        scratch_shapes=[
            pltpu.VMEM((block * heads, 128), f32),
            pltpu.VMEM((heads * block, context), f32),
            pltpu.SemaphoreType.DMA,
        ],
        compiler_params=pltpu.CompilerParams(vmem_limit_bytes=20 << 20),
        name="attend",
    )(
        in_hbm(lengths),
        mine,
        in_hbm(query_latent),
        in_hbm(query_rope),
        in_hbm(cache_latent),
        in_hbm(cache_rope),
        in_hbm(table),
    )
    return [p.reshape(group * tokens, latent) for p in parts], copied


def fetch_tables(tables, after):
    count = len(tables)

    def body(*refs):
        sems = refs[-1]
        outs = refs[-1 - count : -1]
        copies = [pltpu.make_async_copy(refs[i], outs[i], sems.at[i]) for i in range(count)]
        for c in copies:
            c.start()
        for c in copies:
            c.wait()

    return pl.pallas_call(
        body,
        out_shape=[pltpu.VMEM(t.shape, bf16) for t in tables],
        in_specs=[pl.BlockSpec(memory_space=pl.ANY)] * (count + 1),
        out_specs=[pl.BlockSpec(memory_space=pl.ANY)] * count,
        scratch_shapes=[pltpu.SemaphoreType.DMA((count,))],
        compiler_params=pltpu.CompilerParams(vmem_limit_bytes=1 << 20),
        name="fetch_tables",
    )(*[in_hbm(t) for t in tables], after)


def project(parts, value_up, out_proj, tokens, own, before):
    latent, up_width = value_up.shape
    width = out_proj.shape[1]
    head_v = up_width * tokens // parts[0].shape[0]
    pair_count = up_width // 128
    count = len(parts)
    half_rows = count * tokens

    def body(*refs):
        parts_ref = refs[:count]
        up_ref, w_ref = refs[count : count + 2]
        outs = refs[-count:]
        low = lax.broadcasted_iota(jnp.int32, (half_rows, 128), 1) < head_v
        heads = []
        for j in range(pair_count):
            rows = [r[(2 * j + half) * tokens : (2 * j + half + 1) * tokens, :] for half in (0, 1) for r in parts_ref]
            both = nn(jnp.concatenate(rows, axis=0), up_ref[:, 128 * j : 128 * (j + 1)])
            heads.append(jnp.where(low, both[:half_rows], both[half_rows:]).astype(bf16))
        total = nn(jnp.concatenate(heads, axis=1), w_ref[...])
        for i, o in enumerate(outs):
            o[...] = total[i * tokens : (i + 1) * tokens].astype(o.dtype)

    whole = pl.BlockSpec(memory_space=pltpu.VMEM)
    return pl.pallas_call(
        body,
        out_shape=[jax.ShapeDtypeStruct((tokens, width), f32 if own and i == 0 else bf16) for i in range(count)],
        in_specs=[whole] * (count + 2) + [pl.BlockSpec(memory_space=pl.ANY)] * len(before),
        compiler_params=pltpu.CompilerParams(vmem_limit_bytes=16 << 20),
        name="project",
    )(*parts, value_up, out_proj, *before)


def tn(a, b):
    return lax.dot_general(a, b, (((0,), (0,)), ((), ())), preferred_element_type=f32)


def route(expert_ids, affinity, experts):
    top, tokens = expert_ids.shape
    per_expert = SLOTS * QUARTERS
    columns = experts * per_expert

    def body(id_ref, aff_ref, pick_ref, weight_ref):
        expert = lax.broadcasted_iota(jnp.int32, (experts, tokens), 0)
        aff = aff_ref[...]
        weight = route_scale * aff / jnp.sum(aff, axis=0, keepdims=True)
        named = jnp.zeros((experts, tokens), f32)
        spread = jnp.zeros((experts, tokens), f32)
        for k in range(top):
            here = id_ref[k : k + 1, :] == expert
            named = named + jnp.where(here, 1.0, 0.0)
            spread = spread + jnp.where(here, weight[k : k + 1, :], 0.0)
        below = lax.broadcasted_iota(jnp.int32, (tokens, tokens), 0) < lax.broadcasted_iota(jnp.int32, (tokens, tokens), 1)
        earlier = nn(named.astype(bf16), below.astype(f32).astype(bf16))
        column = lax.broadcasted_iota(jnp.int32, (experts, columns), 1)
        widen = (column // per_expert == lax.broadcasted_iota(jnp.int32, (experts, columns), 0)).astype(f32).astype(bf16)
        high = spread.astype(bf16)
        low = (spread - high.astype(f32)).astype(bf16)
        named_wide = tn(named.astype(bf16), widen)
        earlier_wide = tn(earlier.astype(bf16), widen)
        high_wide = tn(high, widen)
        low_wide = tn(low, widen)
        at = lax.broadcasted_iota(jnp.int32, (tokens, columns), 1)
        slot = ((at // QUARTERS) % SLOTS).astype(f32)
        taken = jnp.logical_and(named_wide > 0.5, earlier_wide == slot)
        picks = []
        for q in range(QUARTERS):
            here = jnp.logical_and(taken, at % QUARTERS == q)
            picks.append(jnp.where(here, 1.0, 0.0))
            weight_ref[q * tokens : (q + 1) * tokens, :] = jnp.where(here, high_wide, 0.0).astype(bf16)
            weight_ref[(QUARTERS + q) * tokens : (QUARTERS + q + 1) * tokens, :] = jnp.where(here, low_wide, 0.0).astype(bf16)
        pick_ref[...] = jnp.concatenate(picks, axis=0).T.astype(bf16)

    return pl.pallas_call(
        body,
        out_shape=[
            jax.ShapeDtypeStruct((columns, QUARTERS * tokens), bf16),
            jax.ShapeDtypeStruct((2 * QUARTERS * tokens, columns), bf16),
        ],
        compiler_params=pltpu.CompilerParams(vmem_limit_bytes=8 << 20),
        name="route",
    )(expert_ids, affinity)


def norm_dispatch(own, parts, hidden_in, norm_gain, pick):
    tokens, width = hidden_in.shape
    quarter = width // QUARTERS

    def body(own_ref, p1, p2, p3, h_ref, g_ref, pick_ref, hid_ref, out_ref):
        total = own_ref[...] + p1[...].astype(f32) + p2[...].astype(f32) + p3[...].astype(f32)
        hidden = (h_ref[...].astype(f32) + total).astype(bf16)
        hid_ref[...] = hidden
        wide = hidden.astype(f32)
        inv = lax.rsqrt(jnp.sum(wide * wide, axis=1, keepdims=True) * (1.0 / width) + norm_eps)
        normed = (wide * inv * g_ref[...]).astype(bf16)
        stacked = jnp.concatenate([normed[:, q * quarter : (q + 1) * quarter] for q in range(QUARTERS)], axis=0)
        out_ref[...] = nn(pick_ref[...], stacked).astype(bf16)

    return pl.pallas_call(
        body,
        out_shape=[
            jax.ShapeDtypeStruct((tokens, width), bf16),
            jax.ShapeDtypeStruct((pick.shape[0], quarter), bf16),
        ],
        compiler_params=pltpu.CompilerParams(vmem_limit_bytes=16 << 20),
        name="norm_dispatch",
    )(own, *parts, hidden_in, norm_gain, pick)


def swap_quarters(parts):
    a, b, c, d = parts
    row = lax.broadcasted_iota(jnp.int32, a.shape, a.ndim - 2)
    odd = row % 2 == 1
    upper = (row // 2) % 2 == 1

    def swap(x, y, mask, distance):
        axis = x.ndim - 2
        size = x.shape[axis]
        return (
            jnp.where(mask, pltpu.roll(y, distance, axis), x),
            jnp.where(mask, y, pltpu.roll(x, size - distance, axis)),
        )

    a, b = swap(a, b, odd, 1)
    c, d = swap(c, d, odd, 1)
    a, c = swap(a, c, upper, 2)
    b, d = swap(b, d, upper, 2)
    return a, b, c, d


def run_expert(rows, gate, down):
    total, quarter = rows.shape
    count = total // QUARTERS
    hidden_units = gate.shape[1]
    lanes = quarter // 128
    blocks = count // 8

    def body(r_ref, g_ref, d_ref, o_ref, in_scr, out_scr):
        for c in range(lanes):
            at = slice(128 * c, 128 * (c + 1))
            four = r_ref[:, at].astype(f32).reshape(blocks, QUARTERS, 8, 128)
            for q, part in enumerate(swap_quarters([four[:, q] for q in range(QUARTERS)])):
                in_scr[:, q * quarter + 128 * c : q * quarter + 128 * (c + 1)] = part.reshape(count, 128).astype(bf16)
        inner = nn(in_scr[...], g_ref[...])
        act = (inner / (1.0 + jnp.exp(-inner))).astype(bf16)
        out_scr[...] = nn(act, d_ref[...])
        for c in range(lanes):
            at = slice(128 * c, 128 * (c + 1))
            four = [
                out_scr[:, q * quarter + 128 * c : q * quarter + 128 * (c + 1)].reshape(blocks, 8, 128)
                for q in range(QUARTERS)
            ]
            mixed = jnp.stack(swap_quarters(four), axis=1)
            o_ref[:, at] = mixed.reshape(total, 128).astype(bf16)

    whole = pl.BlockSpec(memory_space=pltpu.VMEM)
    return pl.pallas_call(
        body,
        out_shape=jax.ShapeDtypeStruct((total, quarter), bf16),
        in_specs=[whole] * 3,
        scratch_shapes=[
            pltpu.VMEM((count, QUARTERS * quarter), bf16),
            pltpu.VMEM((count, QUARTERS * quarter), f32),
        ],
        compiler_params=pltpu.CompilerParams(vmem_limit_bytes=32 << 20),
        name="run_expert",
    )(rows, gate, down)


def combine(rows, weight, hidden):
    tokens, width = hidden.shape
    quarter = width // QUARTERS

    def body(r_ref, w_ref, h_ref, o_ref):
        both = nn(w_ref[...], r_ref[...])
        half = QUARTERS * tokens
        moe = both[:half] + both[half:]
        for q in range(QUARTERS):
            at = slice(q * quarter, (q + 1) * quarter)
            o_ref[:, at] = (h_ref[:, at].astype(f32) + moe[q * tokens : (q + 1) * tokens]).astype(bf16)

    return pl.pallas_call(
        body,
        out_shape=jax.ShapeDtypeStruct((tokens, width), bf16),
        compiler_params=pltpu.CompilerParams(vmem_limit_bytes=16 << 20),
        name="combine",
    )(rows, weight, hidden)


def per_device(
    hidden_in,
    query_latent,
    query_rope,
    cache_latent,
    cache_rope,
    lengths,
    value_up,
    out_proj,
    norm_gain,
    expert_gate,
    expert_down,
    expert_ids,
    affinity,
):
    tokens, width = hidden_in.shape
    experts = lax.axis_size("dp") * lax.axis_size("tp")
    mine = lax.axis_index("tp").astype(jnp.int32).reshape(1)

    def shifted(array, shift):
        return lax.ppermute(array, "tp", [(i, (i + shift) % TP) for i in range(TP)])

    pick, weight = route(expert_ids.T, affinity.T, experts)
    by_shift, out_table = attend(lengths, mine, query_latent, query_rope, cache_latent, cache_rope, out_proj, 8)
    gates = fetch_tables([expert_gate[0], expert_down[0]], by_shift[0])
    latents = [by_shift[0]] + [shifted(part, shift) for part, shift in zip(by_shift[1:], SHIFTS[1:])]
    sums = project(latents[:2], value_up, out_table, tokens, True, gates)
    sums = sums + project(latents[2:], value_up, out_table, tokens, False, ())
    parts = [shifted(part, -shift) for part, shift in zip(sums[1:], SHIFTS[1:])]
    hidden, outgoing = norm_dispatch(sums[0], parts, hidden_in, norm_gain.reshape(1, width), pick)

    def exchange(rows):
        cut = rows.reshape(experts, SLOTS * QUARTERS, width // QUARTERS)
        return lax.all_to_all(cut, ("dp", "tp"), 0, 0, tiled=True).reshape(rows.shape)

    answer = run_expert(exchange(outgoing), *gates)
    return combine(exchange(answer), weight, hidden)


def solution(mesh):
    return jax.shard_map(
        per_device,
        mesh=mesh,
        in_specs=(
            P(("dp", "tp"), None),
            P(("dp", "tp"), None, None),
            P(("dp", "tp"), None),
            P(("dp", "tp"), None, None),
            P(("dp", "tp"), None, None),
            P(("dp", "tp")),
            P(None, "tp"),
            P("tp", None),
            P(),
            P(("dp", "tp"), None, None),
            P(("dp", "tp"), None, None),
            P(("dp", "tp"), None),
            P(("dp", "tp"), None),
        ),
        out_specs=P(("dp", "tp"), None),
        check_vma=False,
    )
```

```python
import jax
import jax.numpy as jnp
from jax import lax
from jax.experimental import pallas as pl
from jax.experimental.pallas import tpu as pltpu
from jax.sharding import PartitionSpec as P

score_scale = 192.0 ** (-0.5)
norm_eps = 1e-06
route_scale = 2.5
bf16 = jnp.bfloat16
f32 = jnp.float32


TP = 4
SLOTS = 2
QUARTERS = 4
SHIFTS = (0, 2, 3, 1)


def nn(a, b):
    return lax.dot_general(a, b, (((1,), (0,)), ((), ())), preferred_element_type=f32)


def nt(a, b):
    return lax.dot_general(a, b, (((1,), (1,)), ((), ())), preferred_element_type=f32)


def in_hbm(array):
    return pltpu.with_memory_space_constraint(array, pltpu.HBM)


def attend(lengths, mine, query_latent, query_rope, cache_latent, cache_rope, table, block):
    tokens, heads, latent = query_latent.shape
    context = cache_latent.shape[1]
    rope = cache_rope.shape[1]
    group = heads // TP
    steps = tokens // block
    pairs = heads * rope // 128

    def body(len_ref, mine_ref, q_ref, qr_ref, c_ref, cr_ref, t_ref, o0, o1, o2, o3, copied, qr_scr, w_scr, sem):
        step = pl.program_id(0)
        fetch = pltpu.make_async_copy(t_ref, copied, sem)

        @pl.when(step == 0)
        def _():
            fetch.start()

        for j in range(pairs):
            pair = qr_ref[:, 128 * j : 128 * (j + 1)].astype(f32)
            qr_scr[pl.ds(2 * j, block, stride=heads), :] = pair
            qr_scr[pl.ds(2 * j + 1, block, stride=heads), :] = pltpu.roll(pair, 128 - rope, 1)
        position = lax.broadcasted_iota(jnp.int32, (heads, context), 1)
        for i in range(0, block, 2):
            both = nt(q_ref[i : i + 2].reshape(2 * heads, latent), c_ref[i : i + 2].reshape(2 * context, latent))
            for k in (0, 1):
                t = i + k
                rot = qr_scr[t * heads : (t + 1) * heads, :rope].astype(bf16)
                scores = both[k * heads : (k + 1) * heads, k * context : (k + 1) * context] + nn(rot, cr_ref[t])
                live = position < len_ref[step * block + t]
                w_scr[pl.ds(t, heads, stride=block), :] = jnp.where(live, scores * score_scale, -jnp.inf)
        scores = w_scr[...]
        raised = jnp.exp(scores - jnp.max(scores, axis=1, keepdims=True))
        weights = (raised / jnp.sum(raised, axis=1, keepdims=True)).astype(bf16)
        token = lax.broadcasted_iota(jnp.int32, (heads * block, context), 0) % block
        spread = jnp.concatenate([jnp.where(token == i, weights, jnp.zeros_like(weights)) for i in range(block)], axis=1)
        mixed = nn(spread, c_ref[...].reshape(block * context, latent)).reshape(heads, block, latent).astype(bf16)
        first_token = pl.multiple_of(step * block, block)
        for g in range(TP):
            for shift, o in zip(SHIFTS, (o0, o1, o2, o3)):

                @pl.when(mine_ref[0] ^ shift == g)
                def _():
                    o[:, pl.ds(first_token, block), :] = mixed[g * group : (g + 1) * group]

        @pl.when(step == steps - 1)
        def _():
            fetch.wait()

    out = jax.ShapeDtypeStruct((group, tokens, latent), bf16)
    *parts, copied = pl.pallas_call(
        body,
        out_shape=[out] * TP + [pltpu.VMEM(table.shape, bf16)],
        grid=(steps,),
        in_specs=[
            pl.BlockSpec((tokens,), lambda i: (0,), memory_space=pltpu.SMEM),
            pl.BlockSpec(memory_space=pltpu.SMEM),
            pl.BlockSpec((block, heads, latent), lambda i: (i, 0, 0)),
            pl.BlockSpec((block, heads * rope), lambda i: (i, 0)),
            pl.BlockSpec((block, context, latent), lambda i: (i, 0, 0)),
            pl.BlockSpec((block, rope, context), lambda i: (i, 0, 0)),
            pl.BlockSpec(memory_space=pl.ANY),
        ],
        out_specs=[pl.BlockSpec((group, tokens, latent), lambda i: (0, 0, 0))] * TP + [pl.BlockSpec(memory_space=pl.ANY)],
        scratch_shapes=[
            pltpu.VMEM((block * heads, 128), f32),
            pltpu.VMEM((heads * block, context), f32),
            pltpu.SemaphoreType.DMA,
        ],
        compiler_params=pltpu.CompilerParams(vmem_limit_bytes=20 << 20),
        name="attend",
    )(
        in_hbm(lengths),
        mine,
        in_hbm(query_latent),
        in_hbm(query_rope),
        in_hbm(cache_latent),
        in_hbm(cache_rope),
        in_hbm(table),
    )
    return [p.reshape(group * tokens, latent) for p in parts], copied


def fetch_tables(tables, after):
    count = len(tables)

    def body(*refs):
        sems = refs[-1]
        outs = refs[-1 - count : -1]
        copies = [pltpu.make_async_copy(refs[i], outs[i], sems.at[i]) for i in range(count)]
        for c in copies:
            c.start()
        for c in copies:
            c.wait()

    return pl.pallas_call(
        body,
        out_shape=[pltpu.VMEM(t.shape, bf16) for t in tables],
        in_specs=[pl.BlockSpec(memory_space=pl.ANY)] * (count + 1),
        out_specs=[pl.BlockSpec(memory_space=pl.ANY)] * count,
        scratch_shapes=[pltpu.SemaphoreType.DMA((count,))],
        compiler_params=pltpu.CompilerParams(vmem_limit_bytes=1 << 20),
        name="fetch_tables",
    )(*[in_hbm(t) for t in tables], after)


def project(parts, value_up, out_proj, tokens, own, before):
    latent, up_width = value_up.shape
    width = out_proj.shape[1]
    head_v = up_width * tokens // parts[0].shape[0]
    pair_count = up_width // 128
    count = len(parts)
    half_rows = count * tokens

    def body(*refs):
        parts_ref = refs[:count]
        up_ref, w_ref = refs[count : count + 2]
        outs = refs[-count:]
        low = lax.broadcasted_iota(jnp.int32, (half_rows, 128), 1) < head_v
        heads = []
        for j in range(pair_count):
            rows = [r[(2 * j + half) * tokens : (2 * j + half + 1) * tokens, :] for half in (0, 1) for r in parts_ref]
            both = nn(jnp.concatenate(rows, axis=0), up_ref[:, 128 * j : 128 * (j + 1)])
            heads.append(jnp.where(low, both[:half_rows], both[half_rows:]).astype(bf16))
        total = nn(jnp.concatenate(heads, axis=1), w_ref[...])
        for i, o in enumerate(outs):
            o[...] = total[i * tokens : (i + 1) * tokens].astype(o.dtype)

    whole = pl.BlockSpec(memory_space=pltpu.VMEM)
    return pl.pallas_call(
        body,
        out_shape=[jax.ShapeDtypeStruct((tokens, width), f32 if own and i == 0 else bf16) for i in range(count)],
        in_specs=[whole] * (count + 2) + [pl.BlockSpec(memory_space=pl.ANY)] * len(before),
        compiler_params=pltpu.CompilerParams(vmem_limit_bytes=16 << 20),
        name=f"project_{count}",
    )(*parts, value_up, out_proj, *before)


def tn(a, b):
    return lax.dot_general(a, b, (((0,), (0,)), ((), ())), preferred_element_type=f32)


def route(expert_ids, affinity, experts):
    top, tokens = expert_ids.shape
    per_expert = SLOTS * QUARTERS
    columns = experts * per_expert

    def body(id_ref, aff_ref, pick_ref, weight_ref):
        expert = lax.broadcasted_iota(jnp.int32, (experts, tokens), 0)
        aff = aff_ref[...]
        weight = route_scale * aff / jnp.sum(aff, axis=0, keepdims=True)
        named = jnp.zeros((experts, tokens), f32)
        spread = jnp.zeros((experts, tokens), f32)
        for k in range(top):
            here = id_ref[k : k + 1, :] == expert
            named = named + jnp.where(here, 1.0, 0.0)
            spread = spread + jnp.where(here, weight[k : k + 1, :], 0.0)
        below = lax.broadcasted_iota(jnp.int32, (tokens, tokens), 0) < lax.broadcasted_iota(jnp.int32, (tokens, tokens), 1)
        earlier = nn(named.astype(bf16), below.astype(f32).astype(bf16))
        column = lax.broadcasted_iota(jnp.int32, (experts, columns), 1)
        widen = (column // per_expert == lax.broadcasted_iota(jnp.int32, (experts, columns), 0)).astype(f32).astype(bf16)
        high = spread.astype(bf16)
        low = (spread - high.astype(f32)).astype(bf16)
        named_wide = tn(named.astype(bf16), widen)
        earlier_wide = tn(earlier.astype(bf16), widen)
        high_wide = tn(high, widen)
        low_wide = tn(low, widen)
        at = lax.broadcasted_iota(jnp.int32, (tokens, columns), 1)
        slot = ((at // QUARTERS) % SLOTS).astype(f32)
        taken = jnp.logical_and(named_wide > 0.5, earlier_wide == slot)
        picks = []
        for q in range(QUARTERS):
            here = jnp.logical_and(taken, at % QUARTERS == q)
            picks.append(jnp.where(here, 1.0, 0.0))
            weight_ref[q * tokens : (q + 1) * tokens, :] = jnp.where(here, high_wide, 0.0).astype(bf16)
            weight_ref[(QUARTERS + q) * tokens : (QUARTERS + q + 1) * tokens, :] = jnp.where(here, low_wide, 0.0).astype(bf16)
        pick_ref[...] = jnp.concatenate(picks, axis=0).T.astype(bf16)

    return pl.pallas_call(
        body,
        out_shape=[
            jax.ShapeDtypeStruct((columns, QUARTERS * tokens), bf16),
            jax.ShapeDtypeStruct((2 * QUARTERS * tokens, columns), bf16),
        ],
        compiler_params=pltpu.CompilerParams(vmem_limit_bytes=8 << 20),
        name="route",
    )(expert_ids, affinity)


def norm_dispatch(own, parts, hidden_in, norm_gain, pick):
    tokens, width = hidden_in.shape
    quarter = width // QUARTERS

    def body(own_ref, p1, p2, p3, h_ref, g_ref, pick_ref, hid_ref, out_ref):
        total = own_ref[...] + p1[...].astype(f32) + p2[...].astype(f32) + p3[...].astype(f32)
        hidden = (h_ref[...].astype(f32) + total).astype(bf16)
        hid_ref[...] = hidden
        wide = hidden.astype(f32)
        inv = lax.rsqrt(jnp.sum(wide * wide, axis=1, keepdims=True) * (1.0 / width) + norm_eps)
        normed = (wide * inv * g_ref[...]).astype(bf16)
        stacked = jnp.concatenate([normed[:, q * quarter : (q + 1) * quarter] for q in range(QUARTERS)], axis=0)
        out_ref[...] = nn(pick_ref[...], stacked).astype(bf16)

    return pl.pallas_call(
        body,
        out_shape=[
            jax.ShapeDtypeStruct((tokens, width), bf16),
            jax.ShapeDtypeStruct((pick.shape[0], quarter), bf16),
        ],
        compiler_params=pltpu.CompilerParams(vmem_limit_bytes=16 << 20),
        name="norm_dispatch",
    )(own, *parts, hidden_in, norm_gain, pick)


def swap_quarters(parts):
    a, b, c, d = parts
    row = lax.broadcasted_iota(jnp.int32, a.shape, a.ndim - 2)
    odd = row % 2 == 1
    upper = (row // 2) % 2 == 1

    def swap(x, y, mask, distance):
        axis = x.ndim - 2
        size = x.shape[axis]
        return (
            jnp.where(mask, pltpu.roll(y, distance, axis), x),
            jnp.where(mask, y, pltpu.roll(x, size - distance, axis)),
        )

    a, b = swap(a, b, odd, 1)
    c, d = swap(c, d, odd, 1)
    a, c = swap(a, c, upper, 2)
    b, d = swap(b, d, upper, 2)
    return a, b, c, d


def run_expert(rows, gate, down):
    total, quarter = rows.shape
    count = total // QUARTERS
    lanes = quarter // 128
    blocks = count // 8

    def body(r_ref, g_ref, d_ref, o_ref):
        inner = None
        for c in range(lanes):
            four = r_ref[:, 128 * c : 128 * (c + 1)].astype(f32).reshape(blocks, QUARTERS, 8, 128)
            parts = swap_quarters([four[:, q] for q in range(QUARTERS)])
            lhs = jnp.concatenate([p.reshape(count, 128).astype(bf16) for p in parts], axis=1)
            table = [g_ref[q * quarter + 128 * c : q * quarter + 128 * (c + 1), :] for q in range(QUARTERS)]
            part = nn(lhs, jnp.concatenate(table, axis=0))
            inner = part if inner is None else inner + part
        act = (inner / (1.0 + jnp.exp(-inner))).astype(bf16)
        for c in range(lanes):
            table = [d_ref[:, q * quarter + 128 * c : q * quarter + 128 * (c + 1)] for q in range(QUARTERS)]
            out = nn(act, jnp.concatenate(table, axis=1))
            four = [out[:, 128 * q : 128 * (q + 1)].reshape(blocks, 8, 128) for q in range(QUARTERS)]
            o_ref[:, 128 * c : 128 * (c + 1)] = jnp.stack(swap_quarters(four), axis=1).reshape(total, 128).astype(bf16)

    whole = pl.BlockSpec(memory_space=pltpu.VMEM)
    return pl.pallas_call(
        body,
        out_shape=jax.ShapeDtypeStruct((total, quarter), bf16),
        in_specs=[whole] * 3,
        compiler_params=pltpu.CompilerParams(vmem_limit_bytes=32 << 20),
        name="run_expert",
    )(rows, gate, down)


def combine(rows, weight, hidden):
    tokens, width = hidden.shape
    quarter = width // QUARTERS

    def body(r_ref, w_ref, h_ref, o_ref):
        both = nn(w_ref[...], r_ref[...])
        half = QUARTERS * tokens
        moe = both[:half] + both[half:]
        for q in range(QUARTERS):
            at = slice(q * quarter, (q + 1) * quarter)
            o_ref[:, at] = (h_ref[:, at].astype(f32) + moe[q * tokens : (q + 1) * tokens]).astype(bf16)

    return pl.pallas_call(
        body,
        out_shape=jax.ShapeDtypeStruct((tokens, width), bf16),
        compiler_params=pltpu.CompilerParams(vmem_limit_bytes=16 << 20),
        name="combine",
    )(rows, weight, hidden)


def per_device(
    hidden_in,
    query_latent,
    query_rope,
    cache_latent,
    cache_rope,
    lengths,
    value_up,
    out_proj,
    norm_gain,
    expert_gate,
    expert_down,
    expert_ids,
    affinity,
):
    tokens, width = hidden_in.shape
    experts = lax.axis_size("dp") * lax.axis_size("tp")
    mine = lax.axis_index("tp").astype(jnp.int32).reshape(1)

    def shifted(array, shift):
        return lax.ppermute(array, "tp", [(i, i ^ shift) for i in range(TP)])

    pick, weight = route(expert_ids.T, affinity.T, experts)
    by_shift, out_table = attend(lengths, mine, query_latent, query_rope, cache_latent, cache_rope, out_proj, 8)
    gates = fetch_tables([expert_gate[0], expert_down[0]], by_shift[0])
    latents = [by_shift[0]] + [shifted(part, shift) for part, shift in zip(by_shift[1:], SHIFTS[1:])]
    sums = project(latents[:2], value_up, out_table, tokens, True, gates)
    sums = sums + project(latents[2:3], value_up, out_table, tokens, False, ())
    sums = sums + project(latents[3:], value_up, out_table, tokens, False, ())
    parts = [shifted(part, shift) for part, shift in zip(sums[1:], SHIFTS[1:])]
    hidden, outgoing = norm_dispatch(sums[0], parts, hidden_in, norm_gain.reshape(1, width), pick)

    def exchange(rows):
        cut = rows.reshape(experts, SLOTS * QUARTERS, width // QUARTERS)
        return lax.all_to_all(cut, ("dp", "tp"), 0, 0, tiled=True).reshape(rows.shape)

    answer = run_expert(exchange(outgoing), *gates)
    return combine(exchange(answer), weight, hidden)


def solution(mesh):
    return jax.shard_map(
        per_device,
        mesh=mesh,
        in_specs=(
            P(("dp", "tp"), None),
            P(("dp", "tp"), None, None),
            P(("dp", "tp"), None),
            P(("dp", "tp"), None, None),
            P(("dp", "tp"), None, None),
            P(("dp", "tp")),
            P(None, "tp"),
            P("tp", None),
            P(),
            P(("dp", "tp"), None, None),
            P(("dp", "tp"), None, None),
            P(("dp", "tp"), None),
            P(("dp", "tp"), None),
        ),
        out_specs=P(("dp", "tp"), None),
        check_vma=False,
    )
```

```python
import jax
import jax.numpy as jnp
from jax import lax
from jax.experimental import pallas as pl
from jax.experimental.pallas import tpu as pltpu
from jax.sharding import PartitionSpec as P

score_scale = 192.0 ** (-0.5)
norm_eps = 1e-06
route_scale = 2.5
bf16 = jnp.bfloat16
f32 = jnp.float32


TP = 4
SLOTS = 2
QUARTERS = 4
SHIFTS = (0, 2, 3, 1)


def nn(a, b):
    return lax.dot_general(a, b, (((1,), (0,)), ((), ())), preferred_element_type=f32)


def nt(a, b):
    return lax.dot_general(a, b, (((1,), (1,)), ((), ())), preferred_element_type=f32)


def in_hbm(array):
    return pltpu.with_memory_space_constraint(array, pltpu.HBM)


def attend(lengths, mine, query_latent, query_rope, cache_latent, cache_rope, table, block):
    tokens, heads, latent = query_latent.shape
    context = cache_latent.shape[1]
    rope = cache_rope.shape[1]
    group = heads // TP
    steps = tokens // block
    pairs = heads * rope // 128

    def body(len_ref, mine_ref, q_ref, qr_ref, c_ref, cr_ref, t_ref, o0, o1, o2, o3, copied, qr_scr, w_scr, sem):
        step = pl.program_id(0)
        fetch = pltpu.make_async_copy(t_ref, copied, sem)

        @pl.when(step == 0)
        def _():
            fetch.start()

        for j in range(pairs):
            pair = qr_ref[:, 128 * j : 128 * (j + 1)].astype(f32)
            qr_scr[pl.ds(2 * j, block, stride=heads), :] = pair
            qr_scr[pl.ds(2 * j + 1, block, stride=heads), :] = pltpu.roll(pair, 128 - rope, 1)
        position = lax.broadcasted_iota(jnp.int32, (heads, context), 1)
        for i in range(0, block, 2):
            both = nt(q_ref[i : i + 2].reshape(2 * heads, latent), c_ref[i : i + 2].reshape(2 * context, latent))
            for k in (0, 1):
                t = i + k
                rot = qr_scr[t * heads : (t + 1) * heads, :rope].astype(bf16)
                scores = both[k * heads : (k + 1) * heads, k * context : (k + 1) * context] + nn(rot, cr_ref[t])
                live = position < len_ref[step * block + t]
                w_scr[pl.ds(t, heads, stride=block), :] = jnp.where(live, scores * score_scale, -jnp.inf)
        scores = w_scr[...]
        raised = jnp.exp(scores - jnp.max(scores, axis=1, keepdims=True))
        weights = (raised / jnp.sum(raised, axis=1, keepdims=True)).astype(bf16)
        token = lax.broadcasted_iota(jnp.int32, (heads * block, context), 0) % block
        spread = jnp.concatenate([jnp.where(token == i, weights, jnp.zeros_like(weights)) for i in range(block)], axis=1)
        mixed = nn(spread, c_ref[...].reshape(block * context, latent)).reshape(heads, block, latent).astype(bf16)
        first_token = pl.multiple_of(step * block, block)
        for g in range(TP):
            for shift, o in zip(SHIFTS, (o0, o1, o2, o3)):

                @pl.when(mine_ref[0] ^ shift == g)
                def _():
                    o[:, pl.ds(first_token, block), :] = mixed[g * group : (g + 1) * group]

        @pl.when(step == steps - 1)
        def _():
            fetch.wait()

    out = jax.ShapeDtypeStruct((group, tokens, latent), bf16)
    *parts, copied = pl.pallas_call(
        body,
        out_shape=[out] * TP + [pltpu.VMEM(table.shape, bf16)],
        grid=(steps,),
        in_specs=[
            pl.BlockSpec((tokens,), lambda i: (0,), memory_space=pltpu.SMEM),
            pl.BlockSpec(memory_space=pltpu.SMEM),
            pl.BlockSpec((block, heads, latent), lambda i: (i, 0, 0)),
            pl.BlockSpec((block, heads * rope), lambda i: (i, 0)),
            pl.BlockSpec((block, context, latent), lambda i: (i, 0, 0)),
            pl.BlockSpec((block, rope, context), lambda i: (i, 0, 0)),
            pl.BlockSpec(memory_space=pl.ANY),
        ],
        out_specs=[pl.BlockSpec((group, tokens, latent), lambda i: (0, 0, 0))] * TP + [pl.BlockSpec(memory_space=pl.ANY)],
        scratch_shapes=[
            pltpu.VMEM((block * heads, 128), f32),
            pltpu.VMEM((heads * block, context), f32),
            pltpu.SemaphoreType.DMA,
        ],
        compiler_params=pltpu.CompilerParams(vmem_limit_bytes=20 << 20),
        name="attend",
    )(
        in_hbm(lengths),
        mine,
        in_hbm(query_latent),
        in_hbm(query_rope),
        in_hbm(cache_latent),
        in_hbm(cache_rope),
        in_hbm(table),
    )
    return [p.reshape(group * tokens, latent) for p in parts], copied


def fetch_tables(tables, after):
    count = len(tables)

    def body(*refs):
        sems = refs[-1]
        outs = refs[-1 - count : -1]
        copies = [pltpu.make_async_copy(refs[i], outs[i], sems.at[i]) for i in range(count)]
        for c in copies:
            c.start()
        for c in copies:
            c.wait()

    return pl.pallas_call(
        body,
        out_shape=[pltpu.VMEM(t.shape, bf16) for t in tables],
        in_specs=[pl.BlockSpec(memory_space=pl.ANY)] * (count + 1),
        out_specs=[pl.BlockSpec(memory_space=pl.ANY)] * count,
        scratch_shapes=[pltpu.SemaphoreType.DMA((count,))],
        compiler_params=pltpu.CompilerParams(vmem_limit_bytes=1 << 20),
        name="fetch_tables",
    )(*[in_hbm(t) for t in tables], after)


def project(parts, value_up, out_proj, tokens, own, before):
    latent, up_width = value_up.shape
    width = out_proj.shape[1]
    head_v = up_width * tokens // parts[0].shape[0]
    pair_count = up_width // 128
    count = len(parts)
    half_rows = count * tokens

    def body(*refs):
        parts_ref = refs[:count]
        up_ref, w_ref = refs[count : count + 2]
        outs = refs[-count:]
        low = lax.broadcasted_iota(jnp.int32, (half_rows, 128), 1) < head_v
        heads = []
        for j in range(pair_count):
            rows = [r[(2 * j + half) * tokens : (2 * j + half + 1) * tokens, :] for half in (0, 1) for r in parts_ref]
            both = nn(jnp.concatenate(rows, axis=0), up_ref[:, 128 * j : 128 * (j + 1)])
            heads.append(jnp.where(low, both[:half_rows], both[half_rows:]).astype(bf16))
        total = nn(jnp.concatenate(heads, axis=1), w_ref[...])
        for i, o in enumerate(outs):
            o[...] = total[i * tokens : (i + 1) * tokens].astype(o.dtype)

    whole = pl.BlockSpec(memory_space=pltpu.VMEM)
    return pl.pallas_call(
        body,
        out_shape=[jax.ShapeDtypeStruct((tokens, width), f32 if own and i == 0 else bf16) for i in range(count)],
        in_specs=[whole] * (count + 2) + [pl.BlockSpec(memory_space=pl.ANY)] * len(before),
        compiler_params=pltpu.CompilerParams(vmem_limit_bytes=16 << 20),
        name=f"project_{count}",
    )(*parts, value_up, out_proj, *before)


def tn(a, b):
    return lax.dot_general(a, b, (((0,), (0,)), ((), ())), preferred_element_type=f32)


def route(expert_ids, affinity, experts):
    top, tokens = expert_ids.shape
    per_expert = SLOTS * QUARTERS
    columns = experts * per_expert

    def body(id_ref, aff_ref, pick_ref, weight_ref):
        expert = lax.broadcasted_iota(jnp.int32, (experts, tokens), 0)
        aff = aff_ref[...]
        weight = route_scale * aff / jnp.sum(aff, axis=0, keepdims=True)
        named = jnp.zeros((experts, tokens), f32)
        spread = jnp.zeros((experts, tokens), f32)
        for k in range(top):
            here = id_ref[k : k + 1, :] == expert
            named = named + jnp.where(here, 1.0, 0.0)
            spread = spread + jnp.where(here, weight[k : k + 1, :], 0.0)
        below = lax.broadcasted_iota(jnp.int32, (tokens, tokens), 0) < lax.broadcasted_iota(jnp.int32, (tokens, tokens), 1)
        earlier = nn(named.astype(bf16), below.astype(f32).astype(bf16))
        column = lax.broadcasted_iota(jnp.int32, (experts, columns), 1)
        widen = (column // per_expert == lax.broadcasted_iota(jnp.int32, (experts, columns), 0)).astype(f32).astype(bf16)
        high = spread.astype(bf16)
        low = (spread - high.astype(f32)).astype(bf16)
        named_wide = tn(named.astype(bf16), widen)
        earlier_wide = tn(earlier.astype(bf16), widen)
        high_wide = tn(high, widen)
        low_wide = tn(low, widen)
        at = lax.broadcasted_iota(jnp.int32, (tokens, columns), 1)
        slot = ((at // QUARTERS) % SLOTS).astype(f32)
        taken = jnp.logical_and(named_wide > 0.5, earlier_wide == slot)
        picks = []
        for q in range(QUARTERS):
            here = jnp.logical_and(taken, at % QUARTERS == q)
            picks.append(jnp.where(here, 1.0, 0.0))
            weight_ref[q * tokens : (q + 1) * tokens, :] = jnp.where(here, high_wide, 0.0).astype(bf16)
            weight_ref[(QUARTERS + q) * tokens : (QUARTERS + q + 1) * tokens, :] = jnp.where(here, low_wide, 0.0).astype(bf16)
        pick_ref[...] = jnp.concatenate(picks, axis=0).T.astype(bf16)

    return pl.pallas_call(
        body,
        out_shape=[
            jax.ShapeDtypeStruct((columns, QUARTERS * tokens), bf16),
            jax.ShapeDtypeStruct((2 * QUARTERS * tokens, columns), bf16),
        ],
        compiler_params=pltpu.CompilerParams(vmem_limit_bytes=8 << 20),
        name="route",
    )(expert_ids, affinity)


def norm_dispatch(own, parts, hidden_in, norm_gain, pick):
    tokens, width = hidden_in.shape
    quarter = width // QUARTERS

    def body(own_ref, p1, p2, p3, h_ref, g_ref, pick_ref, hid_ref, out_ref):
        total = own_ref[...] + p1[...].astype(f32) + p2[...].astype(f32) + p3[...].astype(f32)
        hidden = (h_ref[...].astype(f32) + total).astype(bf16)
        hid_ref[...] = hidden
        wide = hidden.astype(f32)
        inv = lax.rsqrt(jnp.sum(wide * wide, axis=1, keepdims=True) * (1.0 / width) + norm_eps)
        normed = (wide * inv * g_ref[...]).astype(bf16)
        stacked = jnp.concatenate([normed[:, q * quarter : (q + 1) * quarter] for q in range(QUARTERS)], axis=0)
        out_ref[...] = nn(pick_ref[...], stacked).astype(bf16)

    return pl.pallas_call(
        body,
        out_shape=[
            jax.ShapeDtypeStruct((tokens, width), bf16),
            jax.ShapeDtypeStruct((pick.shape[0], quarter), bf16),
        ],
        compiler_params=pltpu.CompilerParams(vmem_limit_bytes=16 << 20),
        name="norm_dispatch",
    )(own, *parts, hidden_in, norm_gain, pick)


def swap_quarters(parts):
    a, b, c, d = parts
    row = lax.broadcasted_iota(jnp.int32, a.shape, a.ndim - 2)
    odd = row % 2 == 1
    upper = (row // 2) % 2 == 1

    def swap(x, y, mask, distance):
        axis = x.ndim - 2
        size = x.shape[axis]
        return (
            jnp.where(mask, pltpu.roll(y, distance, axis), x),
            jnp.where(mask, y, pltpu.roll(x, size - distance, axis)),
        )

    a, b = swap(a, b, odd, 1)
    c, d = swap(c, d, odd, 1)
    a, c = swap(a, c, upper, 2)
    b, d = swap(b, d, upper, 2)
    return a, b, c, d


def run_expert(rows, gate, down):
    total, quarter = rows.shape
    count = total // QUARTERS
    lanes = quarter // 128
    blocks = count // 8

    def body(r_ref, g_ref, d_ref, o_ref):
        inner = None
        for first in range(0, lanes, 2):
            sides, table = [], []
            for c in range(first, min(first + 2, lanes)):
                four = r_ref[:, 128 * c : 128 * (c + 1)].astype(f32).reshape(blocks, QUARTERS, 8, 128)
                parts = swap_quarters([four[:, q] for q in range(QUARTERS)])
                sides += [p.reshape(count, 128).astype(bf16) for p in parts]
                table += [g_ref[q * quarter + 128 * c : q * quarter + 128 * (c + 1), :] for q in range(QUARTERS)]
            part = nn(jnp.concatenate(sides, axis=1), jnp.concatenate(table, axis=0))
            inner = part if inner is None else inner + part
        act = (inner / (1.0 + jnp.exp(-inner))).astype(bf16)
        for c in range(lanes):
            table = [d_ref[:, q * quarter + 128 * c : q * quarter + 128 * (c + 1)] for q in range(QUARTERS)]
            out = nn(act, jnp.concatenate(table, axis=1))
            four = [out[:, 128 * q : 128 * (q + 1)].reshape(blocks, 8, 128) for q in range(QUARTERS)]
            o_ref[:, 128 * c : 128 * (c + 1)] = jnp.stack(swap_quarters(four), axis=1).reshape(total, 128).astype(bf16)

    whole = pl.BlockSpec(memory_space=pltpu.VMEM)
    return pl.pallas_call(
        body,
        out_shape=jax.ShapeDtypeStruct((total, quarter), bf16),
        in_specs=[whole] * 3,
        compiler_params=pltpu.CompilerParams(vmem_limit_bytes=32 << 20),
        name="run_expert",
    )(rows, gate, down)


def combine(rows, weight, hidden):
    tokens, width = hidden.shape
    quarter = width // QUARTERS

    def body(r_ref, w_ref, h_ref, o_ref):
        both = nn(w_ref[...], r_ref[...])
        half = QUARTERS * tokens
        moe = both[:half] + both[half:]
        for q in range(QUARTERS):
            at = slice(q * quarter, (q + 1) * quarter)
            o_ref[:, at] = (h_ref[:, at].astype(f32) + moe[q * tokens : (q + 1) * tokens]).astype(bf16)

    return pl.pallas_call(
        body,
        out_shape=jax.ShapeDtypeStruct((tokens, width), bf16),
        compiler_params=pltpu.CompilerParams(vmem_limit_bytes=16 << 20),
        name="combine",
    )(rows, weight, hidden)


def per_device(
    hidden_in,
    query_latent,
    query_rope,
    cache_latent,
    cache_rope,
    lengths,
    value_up,
    out_proj,
    norm_gain,
    expert_gate,
    expert_down,
    expert_ids,
    affinity,
):
    tokens, width = hidden_in.shape
    experts = lax.axis_size("dp") * lax.axis_size("tp")
    mine = lax.axis_index("tp").astype(jnp.int32).reshape(1)

    def shifted(array, shift):
        return lax.ppermute(array, "tp", [(i, i ^ shift) for i in range(TP)])

    pick, weight = route(expert_ids.T, affinity.T, experts)
    by_shift, out_table = attend(lengths, mine, query_latent, query_rope, cache_latent, cache_rope, out_proj, 8)
    gates = fetch_tables([expert_gate[0], expert_down[0]], by_shift[0])
    latents = [by_shift[0]] + [shifted(part, shift) for part, shift in zip(by_shift[1:], SHIFTS[1:])]
    sums = []
    for at in range(1, TP):
        before = gates if at == 1 else ()
        sums += project(latents[at : at + 1], value_up, out_table, tokens, False, before)
    parts = [shifted(part, shift) for part, shift in zip(sums, SHIFTS[1:])]
    own = project(latents[:1], value_up, out_table, tokens, True, (sums[-1],))
    hidden, outgoing = norm_dispatch(own[0], parts, hidden_in, norm_gain.reshape(1, width), pick)

    def exchange(rows):
        cut = rows.reshape(experts, SLOTS * QUARTERS, width // QUARTERS)
        return lax.all_to_all(cut, ("dp", "tp"), 0, 0, tiled=True).reshape(rows.shape)

    answer = run_expert(exchange(outgoing), *gates)
    return combine(exchange(answer), weight, hidden)


def solution(mesh):
    return jax.shard_map(
        per_device,
        mesh=mesh,
        in_specs=(
            P(("dp", "tp"), None),
            P(("dp", "tp"), None, None),
            P(("dp", "tp"), None),
            P(("dp", "tp"), None, None),
            P(("dp", "tp"), None, None),
            P(("dp", "tp")),
            P(None, "tp"),
            P("tp", None),
            P(),
            P(("dp", "tp"), None, None),
            P(("dp", "tp"), None, None),
            P(("dp", "tp"), None),
            P(("dp", "tp"), None),
        ),
        out_specs=P(("dp", "tp"), None),
        check_vma=False,
    )
```

```python
import jax
import jax.numpy as jnp
from jax import lax
from jax.experimental import pallas as pl
from jax.experimental.pallas import tpu as pltpu
from jax.sharding import PartitionSpec as P

score_scale = 192.0 ** (-0.5)
norm_eps = 1e-06
route_scale = 2.5
bf16 = jnp.bfloat16
f32 = jnp.float32


TP = 4
SLOTS = 2
QUARTERS = 4
SHIFTS = (0, 2, 3, 1)


def nn(a, b):
    return lax.dot_general(a, b, (((1,), (0,)), ((), ())), preferred_element_type=f32)


def nt(a, b):
    return lax.dot_general(a, b, (((1,), (1,)), ((), ())), preferred_element_type=f32)


def in_hbm(array):
    return pltpu.with_memory_space_constraint(array, pltpu.HBM)


def attend(lengths, mine, query_latent, query_rope, cache_latent, cache_rope, table, block):
    tokens, heads, latent = query_latent.shape
    context = cache_latent.shape[1]
    rope = cache_rope.shape[1]
    group = heads // TP
    steps = tokens // block
    pairs = heads * rope // 128

    def body(len_ref, mine_ref, q_ref, qr_ref, c_ref, cr_ref, t_ref, o0, o1, o2, o3, copied, qr_scr, w_scr, sem):
        step = pl.program_id(0)
        fetch = pltpu.make_async_copy(t_ref, copied, sem)

        @pl.when(step == 0)
        def _():
            fetch.start()

        for j in range(pairs):
            pair = qr_ref[:, 128 * j : 128 * (j + 1)].astype(f32)
            qr_scr[pl.ds(2 * j, block, stride=heads), :] = pair
            qr_scr[pl.ds(2 * j + 1, block, stride=heads), :] = pltpu.roll(pair, 128 - rope, 1)
        position = lax.broadcasted_iota(jnp.int32, (heads, context), 1)
        for i in range(0, block, 2):
            both = nt(q_ref[i : i + 2].reshape(2 * heads, latent), c_ref[i : i + 2].reshape(2 * context, latent))
            for k in (0, 1):
                t = i + k
                rot = qr_scr[t * heads : (t + 1) * heads, :rope].astype(bf16)
                scores = both[k * heads : (k + 1) * heads, k * context : (k + 1) * context] + nn(rot, cr_ref[t])
                live = position < len_ref[step * block + t]
                w_scr[pl.ds(t, heads, stride=block), :] = jnp.where(live, scores * score_scale, -jnp.inf)
        scores = w_scr[...]
        raised = jnp.exp(scores - jnp.max(scores, axis=1, keepdims=True))
        weights = (raised / jnp.sum(raised, axis=1, keepdims=True)).astype(bf16)
        token = lax.broadcasted_iota(jnp.int32, (heads * block, context), 0) % block
        spread = jnp.concatenate([jnp.where(token == i, weights, jnp.zeros_like(weights)) for i in range(block)], axis=1)
        mixed = nn(spread, c_ref[...].reshape(block * context, latent)).reshape(heads, block, latent).astype(bf16)
        first_token = pl.multiple_of(step * block, block)
        for g in range(TP):
            for shift, o in zip(SHIFTS, (o0, o1, o2, o3)):

                @pl.when(mine_ref[0] ^ shift == g)
                def _():
                    o[:, pl.ds(first_token, block), :] = mixed[g * group : (g + 1) * group]

        @pl.when(step == steps - 1)
        def _():
            fetch.wait()

    out = jax.ShapeDtypeStruct((group, tokens, latent), bf16)
    *parts, copied = pl.pallas_call(
        body,
        out_shape=[out] * TP + [pltpu.VMEM(table.shape, bf16)],
        grid=(steps,),
        in_specs=[
            pl.BlockSpec((tokens,), lambda i: (0,), memory_space=pltpu.SMEM),
            pl.BlockSpec(memory_space=pltpu.SMEM),
            pl.BlockSpec((block, heads, latent), lambda i: (i, 0, 0)),
            pl.BlockSpec((block, heads * rope), lambda i: (i, 0)),
            pl.BlockSpec((block, context, latent), lambda i: (i, 0, 0)),
            pl.BlockSpec((block, rope, context), lambda i: (i, 0, 0)),
            pl.BlockSpec(memory_space=pl.ANY),
        ],
        out_specs=[pl.BlockSpec((group, tokens, latent), lambda i: (0, 0, 0))] * TP + [pl.BlockSpec(memory_space=pl.ANY)],
        scratch_shapes=[
            pltpu.VMEM((block * heads, 128), f32),
            pltpu.VMEM((heads * block, context), f32),
            pltpu.SemaphoreType.DMA,
        ],
        compiler_params=pltpu.CompilerParams(vmem_limit_bytes=20 << 20),
        name="attend",
    )(
        in_hbm(lengths),
        mine,
        in_hbm(query_latent),
        in_hbm(query_rope),
        in_hbm(cache_latent),
        in_hbm(cache_rope),
        in_hbm(table),
    )
    return [p.reshape(group * tokens, latent) for p in parts], copied


def fetch_tables(tables, after):
    count = len(tables)

    def body(*refs):
        sems = refs[-1]
        outs = refs[-1 - count : -1]
        copies = [pltpu.make_async_copy(refs[i], outs[i], sems.at[i]) for i in range(count)]
        for c in copies:
            c.start()
        for c in copies:
            c.wait()

    return pl.pallas_call(
        body,
        out_shape=[pltpu.VMEM(t.shape, bf16) for t in tables],
        in_specs=[pl.BlockSpec(memory_space=pl.ANY)] * (count + 1),
        out_specs=[pl.BlockSpec(memory_space=pl.ANY)] * count,
        scratch_shapes=[pltpu.SemaphoreType.DMA((count,))],
        compiler_params=pltpu.CompilerParams(vmem_limit_bytes=1 << 20),
        name="fetch_tables",
    )(*[in_hbm(t) for t in tables], after)


def project(parts, value_up, out_proj, tokens, own, before):
    latent, up_width = value_up.shape
    width = out_proj.shape[1]
    head_v = up_width * tokens // parts[0].shape[0]
    pair_count = up_width // 128
    count = len(parts)
    half_rows = count * tokens

    def body(*refs):
        parts_ref = refs[:count]
        up_ref, w_ref = refs[count : count + 2]
        outs = refs[-count:]
        low = lax.broadcasted_iota(jnp.int32, (half_rows, 128), 1) < head_v
        heads = []
        for j in range(pair_count):
            rows = [r[(2 * j + half) * tokens : (2 * j + half + 1) * tokens, :] for half in (0, 1) for r in parts_ref]
            both = nn(jnp.concatenate(rows, axis=0), up_ref[:, 128 * j : 128 * (j + 1)])
            heads.append(jnp.where(low, both[:half_rows], both[half_rows:]).astype(bf16))
        total = nn(jnp.concatenate(heads, axis=1), w_ref[...])
        for i, o in enumerate(outs):
            o[...] = total[i * tokens : (i + 1) * tokens].astype(o.dtype)

    whole = pl.BlockSpec(memory_space=pltpu.VMEM)
    return pl.pallas_call(
        body,
        out_shape=[jax.ShapeDtypeStruct((tokens, width), f32 if own and i == 0 else bf16) for i in range(count)],
        in_specs=[whole] * (count + 2) + [pl.BlockSpec(memory_space=pl.ANY)] * len(before),
        compiler_params=pltpu.CompilerParams(vmem_limit_bytes=16 << 20),
        name=f"project_{count}",
    )(*parts, value_up, out_proj, *before)


def tn(a, b):
    return lax.dot_general(a, b, (((0,), (0,)), ((), ())), preferred_element_type=f32)


def route(expert_ids, affinity, experts):
    top, tokens = expert_ids.shape
    per_expert = SLOTS * QUARTERS
    columns = experts * per_expert

    def body(id_ref, aff_ref, pick_ref, weight_ref):
        expert = lax.broadcasted_iota(jnp.int32, (experts, tokens), 0)
        aff = aff_ref[...]
        weight = route_scale * aff / jnp.sum(aff, axis=0, keepdims=True)
        named = jnp.zeros((experts, tokens), f32)
        spread = jnp.zeros((experts, tokens), f32)
        for k in range(top):
            here = id_ref[k : k + 1, :] == expert
            named = named + jnp.where(here, 1.0, 0.0)
            spread = spread + jnp.where(here, weight[k : k + 1, :], 0.0)
        below = lax.broadcasted_iota(jnp.int32, (tokens, tokens), 0) < lax.broadcasted_iota(jnp.int32, (tokens, tokens), 1)
        earlier = nn(named.astype(bf16), below.astype(f32).astype(bf16))
        column = lax.broadcasted_iota(jnp.int32, (experts, columns), 1)
        widen = (column // per_expert == lax.broadcasted_iota(jnp.int32, (experts, columns), 0)).astype(f32).astype(bf16)
        high = spread.astype(bf16)
        low = (spread - high.astype(f32)).astype(bf16)
        named_wide = tn(named.astype(bf16), widen)
        earlier_wide = tn(earlier.astype(bf16), widen)
        high_wide = tn(high, widen)
        low_wide = tn(low, widen)
        at = lax.broadcasted_iota(jnp.int32, (tokens, columns), 1)
        slot = ((at // QUARTERS) % SLOTS).astype(f32)
        taken = jnp.logical_and(named_wide > 0.5, earlier_wide == slot)
        picks = []
        for q in range(QUARTERS):
            here = jnp.logical_and(taken, at % QUARTERS == q)
            picks.append(jnp.where(here, 1.0, 0.0))
            weight_ref[q * tokens : (q + 1) * tokens, :] = jnp.where(here, high_wide, 0.0).astype(bf16)
            weight_ref[(QUARTERS + q) * tokens : (QUARTERS + q + 1) * tokens, :] = jnp.where(here, low_wide, 0.0).astype(bf16)
        pick_ref[...] = jnp.concatenate(picks, axis=0).T.astype(bf16)

    return pl.pallas_call(
        body,
        out_shape=[
            jax.ShapeDtypeStruct((columns, QUARTERS * tokens), bf16),
            jax.ShapeDtypeStruct((2 * QUARTERS * tokens, columns), bf16),
        ],
        compiler_params=pltpu.CompilerParams(vmem_limit_bytes=8 << 20),
        name="route",
    )(expert_ids, affinity)


def norm_dispatch(own, parts, hidden_in, norm_gain, pick, before):
    tokens, width = hidden_in.shape
    quarter = width // QUARTERS

    def body(own_ref, p1, p2, p3, h_ref, g_ref, pick_ref, _, hid_ref, out_ref):
        total = own_ref[...] + p1[...].astype(f32) + p2[...].astype(f32) + p3[...].astype(f32)
        hidden = (h_ref[...].astype(f32) + total).astype(bf16)
        hid_ref[...] = hidden
        wide = hidden.astype(f32)
        inv = lax.rsqrt(jnp.sum(wide * wide, axis=1, keepdims=True) * (1.0 / width) + norm_eps)
        normed = (wide * inv * g_ref[...]).astype(bf16)
        stacked = jnp.concatenate([normed[:, q * quarter : (q + 1) * quarter] for q in range(QUARTERS)], axis=0)
        out_ref[...] = nn(pick_ref[...], stacked).astype(bf16)

    return pl.pallas_call(
        body,
        out_shape=[
            jax.ShapeDtypeStruct((tokens, width), bf16),
            jax.ShapeDtypeStruct((pick.shape[0], quarter), bf16),
        ],
        in_specs=[pl.BlockSpec(memory_space=pltpu.VMEM)] * 7 + [pl.BlockSpec(memory_space=pl.ANY)],
        compiler_params=pltpu.CompilerParams(vmem_limit_bytes=16 << 20),
        name="norm_dispatch",
    )(own, *parts, hidden_in, norm_gain, pick, before)


def swap_quarters(parts):
    a, b, c, d = parts
    row = lax.broadcasted_iota(jnp.int32, a.shape, a.ndim - 2)
    odd = row % 2 == 1
    upper = (row // 2) % 2 == 1

    def swap(x, y, mask, distance):
        axis = x.ndim - 2
        size = x.shape[axis]
        return (
            jnp.where(mask, pltpu.roll(y, distance, axis), x),
            jnp.where(mask, y, pltpu.roll(x, size - distance, axis)),
        )

    a, b = swap(a, b, odd, 1)
    c, d = swap(c, d, odd, 1)
    a, c = swap(a, c, upper, 2)
    b, d = swap(b, d, upper, 2)
    return a, b, c, d


def run_expert(rows, gate, down):
    total, quarter = rows.shape
    count = total // QUARTERS
    lanes = quarter // 128
    blocks = count // 8

    def body(r_ref, g_ref, d_ref, o_ref):
        inner = None
        for c in range(lanes):
            four = r_ref[:, 128 * c : 128 * (c + 1)].astype(f32).reshape(blocks, QUARTERS, 8, 128)
            parts = swap_quarters([four[:, q] for q in range(QUARTERS)])
            lhs = jnp.concatenate([p.reshape(count, 128).astype(bf16) for p in parts], axis=1)
            table = [g_ref[q * quarter + 128 * c : q * quarter + 128 * (c + 1), :] for q in range(QUARTERS)]
            part = nn(lhs, jnp.concatenate(table, axis=0))
            inner = part if inner is None else inner + part
        act = (inner / (1.0 + jnp.exp(-inner))).astype(bf16)
        for c in range(lanes):
            table = [d_ref[:, q * quarter + 128 * c : q * quarter + 128 * (c + 1)] for q in range(QUARTERS)]
            out = nn(act, jnp.concatenate(table, axis=1))
            four = [out[:, 128 * q : 128 * (q + 1)].reshape(blocks, 8, 128) for q in range(QUARTERS)]
            o_ref[:, 128 * c : 128 * (c + 1)] = jnp.stack(swap_quarters(four), axis=1).reshape(total, 128).astype(bf16)

    whole = pl.BlockSpec(memory_space=pltpu.VMEM)
    return pl.pallas_call(
        body,
        out_shape=jax.ShapeDtypeStruct((total, quarter), bf16),
        in_specs=[whole] * 3,
        compiler_params=pltpu.CompilerParams(vmem_limit_bytes=32 << 20),
        name="run_expert",
    )(rows, gate, down)


def combine(rows, weight, hidden):
    tokens, width = hidden.shape
    quarter = width // QUARTERS

    def body(r_ref, w_ref, h_ref, o_ref):
        both = nn(w_ref[...], r_ref[...])
        half = QUARTERS * tokens
        moe = both[:half] + both[half:]
        for q in range(QUARTERS):
            at = slice(q * quarter, (q + 1) * quarter)
            o_ref[:, at] = (h_ref[:, at].astype(f32) + moe[q * tokens : (q + 1) * tokens]).astype(bf16)

    return pl.pallas_call(
        body,
        out_shape=jax.ShapeDtypeStruct((tokens, width), bf16),
        compiler_params=pltpu.CompilerParams(vmem_limit_bytes=16 << 20),
        name="combine",
    )(rows, weight, hidden)


def per_device(
    hidden_in,
    query_latent,
    query_rope,
    cache_latent,
    cache_rope,
    lengths,
    value_up,
    out_proj,
    norm_gain,
    expert_gate,
    expert_down,
    expert_ids,
    affinity,
):
    tokens, width = hidden_in.shape
    experts = lax.axis_size("dp") * lax.axis_size("tp")
    mine = lax.axis_index("tp").astype(jnp.int32).reshape(1)

    def shifted(array, shift):
        return lax.ppermute(array, "tp", [(i, i ^ shift) for i in range(TP)])

    pick, weight = route(expert_ids.T, affinity.T, experts)
    by_shift, out_table = attend(lengths, mine, query_latent, query_rope, cache_latent, cache_rope, out_proj, 8)
    gates = fetch_tables([expert_gate[0]], by_shift[0])
    latents = [by_shift[0]] + [shifted(part, shift) for part, shift in zip(by_shift[1:], SHIFTS[1:])]
    sums = project(latents[:2], value_up, out_table, tokens, True, gates)
    sums = sums + project(latents[2:3], value_up, out_table, tokens, False, ())
    sums = sums + project(latents[3:], value_up, out_table, tokens, False, ())
    parts = [shifted(part, shift) for part, shift in zip(sums[1:], SHIFTS[1:])]
    downs = fetch_tables([expert_down[0]], sums[-1])
    hidden, outgoing = norm_dispatch(sums[0], parts, hidden_in, norm_gain.reshape(1, width), pick, downs[0])

    def exchange(rows):
        cut = rows.reshape(experts, SLOTS * QUARTERS, width // QUARTERS)
        return lax.all_to_all(cut, ("dp", "tp"), 0, 0, tiled=True).reshape(rows.shape)

    answer = run_expert(exchange(outgoing), *gates, *downs)
    return combine(exchange(answer), weight, hidden)


def solution(mesh):
    return jax.shard_map(
        per_device,
        mesh=mesh,
        in_specs=(
            P(("dp", "tp"), None),
            P(("dp", "tp"), None, None),
            P(("dp", "tp"), None),
            P(("dp", "tp"), None, None),
            P(("dp", "tp"), None, None),
            P(("dp", "tp")),
            P(None, "tp"),
            P("tp", None),
            P(),
            P(("dp", "tp"), None, None),
            P(("dp", "tp"), None, None),
            P(("dp", "tp"), None),
            P(("dp", "tp"), None),
        ),
        out_specs=P(("dp", "tp"), None),
        check_vma=False,
    )
```
